32 devices in a mesh: img: 4 (over x, core), slab: 8 (over z, y).
Axes of the slice: x: 2, y: 2, z: 4, core: 2. Of those that a mesh axis runs over, the one named last changes fastest.
Arguments:
- section_input: bfloat16 [256, 256, 1024], P(('img', 'slab')), parts along dimension 0, may hold values from -54 to 54
- w_reduce: bfloat16 [3, 1024, 256], replicated, may hold values from -0.1875 to 0.1875
- w_spatial: bfloat16 [3, 9, 256, 256], replicated, may hold values from -0.125 to 0.125
- w_expand: bfloat16 [3, 256, 1024], replicated, may hold values from -0.375 to 0.375
- gain_mid: float32 [3, 2, 256], replicated, may hold values from 0.25 to 1.75
- shift_mid: float32 [3, 2, 256], replicated, may hold values from -3 to 3
- gain_out: float32 [3, 1024], replicated, may hold values from 0.25 to 1.75
- shift_out: float32 [3, 1024], replicated, may hold values from -3 to 3
Outputs:
- section_output: bfloat16 [256, 256, 1024], P(('img', 'slab')), parts along dimension 0
The draws below stay inside these ranges and needn't reach their ends.
There are 4 independent parts, one for each index of `img`. The reference program is written for one: setup_inputs(seed, part) draws one part's arguments, and reference() takes and returns one part's arrays. A program takes and returns all parts, laid end to end along the dimension named above; an argument that names none is the same for every part. Nothing has to cross between parts.
All inputs are finite; a program needn't handle non-finite values.
Results may differ from the reference program's by a relative error of at most 0.01.
Values may be sent and summed in bfloat16 or wider, within the bound.
A program may use at most 128 MiB of HBM per device.

```python
import jax
import jax.numpy as jnp
from jax import lax

C = 1024
CM = 256
W = 256
LAYERS = 3
H = 64


def draw_section_input(key, part):
    positions = jnp.arange(H, dtype=jnp.float32) / max(H - 1, 1)
    noise = jnp.clip(jax.random.normal(key, (H, W, C), jnp.float32), -6.0, 6.0)
    scale = jnp.exp(positions * jnp.log(3.0))
    return (noise * scale[:, None, None]).astype(jnp.bfloat16)


def scatter_about(rng, shape, scale, most, held_as=jnp.bfloat16):
    return jnp.clip(scale * jax.random.normal(rng, shape, jnp.float32), -most, most).astype(held_as)


def setup_inputs(seed: int = 0, part: int = 0) -> dict:
    arg_keys = jax.random.split(jax.random.key(seed), 9)
    part_splits = jax.random.split(jax.random.fold_in(arg_keys[8], part), 9)
    return {
        "section_input": draw_section_input(jax.random.fold_in(jax.random.fold_in(arg_keys[8], part), 71), part),
        "w_reduce": scatter_about(arg_keys[1], (LAYERS, C, CM), C ** -0.5, 0.1875),
        "w_spatial": scatter_about(arg_keys[2], (LAYERS, 9, CM, CM), (9 * CM) ** -0.5, 0.125),
        "w_expand": scatter_about(arg_keys[3], (LAYERS, CM, C), CM ** -0.5, 0.375),
        "gain_mid": jnp.clip(1.0 + 0.15 * jax.random.normal(arg_keys[4], (LAYERS, 2, CM), jnp.float32), 0.25, 1.75),
        "shift_mid": scatter_about(arg_keys[5], (LAYERS, 2, CM), 0.5, 3.0, jnp.float32),
        "gain_out": jnp.clip(1.0 + 0.15 * jax.random.normal(arg_keys[6], (LAYERS, C), jnp.float32), 0.25, 1.75),
        "shift_out": scatter_about(arg_keys[7], (LAYERS, C), 0.5, 3.0, jnp.float32),
    }


def normalize(values, gain, shift):
    mean = lax.optimization_barrier(jnp.mean(values, axis=0))
    var = lax.optimization_barrier(jnp.mean(jnp.square(values - mean), axis=0))
    return (values - mean) * jax.lax.rsqrt(var + 1e-05) * gain + shift

def spatial_conv(hidden, taps):
    rows, width, mid = hidden.shape
    padded = jnp.pad(hidden, ((1, 1), (1, 1), (0, 0)))
    total = jnp.zeros((rows * width, taps.shape[2]), jnp.float32)
    for down in range(3):
        for across in range(3):
            window = padded[down:down + rows, across:across + width].reshape(-1, mid)
            total = total + jnp.dot(window, taps[3 * down + across], preferred_element_type=jnp.float32)
    return total

def reference(section_input, w_reduce, w_spatial, w_expand, gain_mid, shift_mid, gain_out, shift_out):
    rows, width, chans = section_input.shape
    mid = w_reduce.shape[2]
    current = section_input
    for layer in range(LAYERS):
        flat = current.reshape(-1, chans)
        reduced = jnp.dot(flat, w_reduce[layer], preferred_element_type=jnp.float32)
        hidden = jnp.maximum(normalize(reduced, gain_mid[layer, 0], shift_mid[layer, 0]), 0.0).astype(jnp.bfloat16)
        spatial = spatial_conv(hidden.reshape(rows, width, mid), w_spatial[layer])
        inner = jnp.maximum(normalize(spatial, gain_mid[layer, 1], shift_mid[layer, 1]), 0.0).astype(jnp.bfloat16)
        expanded = jnp.dot(inner, w_expand[layer], preferred_element_type=jnp.float32)
        summed = normalize(expanded, gain_out[layer], shift_out[layer]) + flat.astype(jnp.float32)
        current = jnp.maximum(summed, 0.0).astype(jnp.bfloat16).reshape(rows, width, chans)
    return current
```

```python
import functools

import jax
import jax.numpy as jnp
from jax import lax
from jax.experimental import pallas as pl
from jax.experimental.pallas import tpu as pltpu
from jax.sharding import PartitionSpec as P

MESH = pl.DeviceIdType.MESH
EPS = 1e-05


def kernel(
    n, x_hbm, wr_hbm, ws_hbm, we_hbm, gain_mid, shift_mid, gain_out, shift_out, out_hbm,
    x, wr, ws, we, red, taps, inner, expanded, halo_out, halo_in, stat_out, stat,
    x_sem, w_sem, out_sem, halo_send, halo_recv, stat_send, stat_recv,
):
    rows, width, chans = x.shape
    layers, _, mid = wr.shape
    chunks = chans // mid
    stages = 2 + chunks
    step = 2 if rows % 2 == 0 else 1
    me = lax.axis_index("slab")
    inv_local = 1.0 / (rows * width)
    inv_count = 1.0 / (rows * width * n)

    def peer(k):
        return lax.rem(me + k, n)

    barrier = pltpu.get_barrier_semaphore()
    for k in range(1, n):
        pl.semaphore_signal(barrier, inc=1, device_id={"slab": peer(k)}, device_id_type=MESH)

    def weight_copy(kind, layer):
        source, target = ((wr_hbm, wr), (ws_hbm, ws), (we_hbm, we))[kind]
        return pltpu.make_async_copy(source.at[layer], target.at[layer], w_sem.at[kind, layer])

    def x_copy(row):
        return pltpu.make_async_copy(x_hbm.at[row], x.at[row], x_sem.at[row])

    def out_copy(chunk):
        cols = pl.ds(chunk * mid, mid)
        return pltpu.make_async_copy(x.at[:, :, cols], out_hbm.at[:, :, cols], out_sem.at[chunk])

    weight_copy(0, 0).start()
    for row in range(rows):
        x_copy(row).start()

    def stat_copy(stage, k):
        return pltpu.make_async_remote_copy(
            src_ref=stat_out.at[stage],
            dst_ref=stat.at[stage, me],
            send_sem=stat_send.at[stage, k],
            recv_sem=stat_recv.at[stage, me],
            device_id={"slab": peer(k)},
            device_id_type=MESH,
        )

    def stat_arrival(stage, k):
        source = peer(k)
        return pltpu.make_async_remote_copy(
            src_ref=stat_out.at[stage],
            dst_ref=stat.at[stage, source],
            send_sem=stat_send.at[stage, k],
            recv_sem=stat_recv.at[stage, source],
            device_id={"slab": source},
            device_id_type=MESH,
        )

    def fold(carry, y):
        total, squares = carry
        y = y.reshape(-1, 8, mid)
        return total + jnp.sum(y, axis=0), squares + jnp.sum(y * y, axis=0)

    def zeros():
        return jnp.zeros((8, mid), jnp.float32), jnp.zeros((8, mid), jnp.float32)

    def send_stats(stage, carry):
        total = jnp.sum(carry[0], axis=0, keepdims=True)
        squares = jnp.sum(carry[1], axis=0, keepdims=True)
        both = jnp.concatenate([total, squares], axis=0)
        stat_out[stage] = both
        stat[stage, me] = both
        for k in range(1, n):
            stat_copy(stage, k).start()
        return total

    def affine(stage, gain, shift):
        for k in range(1, n):
            stat_copy(stage, k).wait_send()
            stat_arrival(stage, k).wait_recv()
        both = jnp.sum(stat[stage], axis=0)
        mean = both[0:1] * inv_count
        var = jnp.maximum(both[1:2] * inv_count - mean * mean, 0.0)
        scale = lax.rsqrt(var + EPS) * gain
        return scale, shift - mean * scale

    def halo_copy(layer, side):
        return pltpu.make_async_remote_copy(
            src_ref=halo_out.at[layer, side],
            dst_ref=halo_in.at[layer, 1 - side],
            send_sem=halo_send.at[layer, side],
            recv_sem=halo_recv.at[layer, 1 - side],
            device_id={"slab": peer(n - 1 if side == 0 else 1)},
            device_id_type=MESH,
        )

    def halo_arrival(layer, side):
        return pltpu.make_async_remote_copy(
            src_ref=halo_out.at[layer, side],
            dst_ref=halo_in.at[layer, side],
            send_sem=halo_send.at[layer, side],
            recv_sem=halo_recv.at[layer, side],
            device_id={"slab": peer(n - 1 if side == 0 else 1)},
            device_id_type=MESH,
        )

    def has_neighbour(side):
        return me > 0 if side == 0 else me < n - 1

    column = lax.broadcasted_iota(jnp.int32, (width, mid), 0)

    def store_taps(row, h):
        at = pl.ds(row * width, width)
        before = jnp.where(column == 0, 0.0, pltpu.roll(h, 1, 0))
        after = jnp.where(column == width - 1, 0.0, pltpu.roll(h, width - 1, 0))
        taps[at, 0:mid] = before.astype(jnp.bfloat16)
        taps[at, mid : 2 * mid] = h.astype(jnp.bfloat16)
        taps[at, 2 * mid : 3 * mid] = after.astype(jnp.bfloat16)

    def layer_step(layer, _):
        first = layer * stages

        weight_copy(0, layer).wait()

        def reduce_step(i, carry):
            @pl.when(layer == 0)
            def _():
                for r in range(step):
                    x_copy(i * step + r).wait()

            y = jnp.dot(
                x[pl.ds(i * step, step)].reshape(step * width, chans),
                wr[layer],
                preferred_element_type=jnp.float32,
            )
            red[pl.ds(i * step * width, step * width), :] = y
            return fold(carry, y)

        carry = lax.fori_loop(0, rows // step, reduce_step, zeros())

        @pl.when(layer == 0)
        def _():
            pl.semaphore_wait(barrier, n - 1)

        local_mean = send_stats(first, carry) * inv_local
        for side in range(2):
            row = 0 if side == 0 else rows - 1
            halo_out[layer, side] = (red[row * width : (row + 1) * width, :] - local_mean).astype(
                jnp.bfloat16
            )

            @pl.when(has_neighbour(side))
            def _():
                halo_copy(layer, side).start()

        weight_copy(1, layer).start()
        weight_copy(2, layer).start()

        @pl.when(layer < layers - 1)
        def _():
            weight_copy(0, layer + 1).start()

        scale, shift = affine(first, gain_mid[layer, 0:1], shift_mid[layer, 0:1])

        def hidden_step(i, _):
            y = red[pl.ds(i * width, width), :]
            store_taps(i + 1, jnp.maximum(y * scale + shift, 0.0))
            return 0

        lax.fori_loop(0, rows, hidden_step, 0)

        weight_copy(1, layer).wait()

        def conv(row, count):
            total = None
            for down in range(3):
                part = jnp.dot(
                    taps[pl.ds((row + down) * width, count * width), :],
                    ws[layer, pl.ds(3 * down, 3)].reshape(3 * mid, mid),
                    preferred_element_type=jnp.float32,
                )
                total = part if total is None else total + part
            red[pl.ds(row * width, count * width), :] = total
            return total

        def inside_step(i, carry):
            return fold(carry, conv(1 + i * step, step))

        carry = lax.fori_loop(0, (rows - 2) // step, inside_step, zeros())

        for side in range(2):
            source = peer(n - 1 if side == 0 else 1)
            row = 0 if side == 0 else rows + 1

            @pl.when(has_neighbour(side))
            def _():
                halo_copy(layer, side).wait_send()
                halo_arrival(layer, side).wait_recv()
                theirs = stat[first, source][0:1] * inv_local
                y = halo_in[layer, side].astype(jnp.float32) + theirs
                store_taps(row, jnp.maximum(y * scale + shift, 0.0))

            @pl.when(jnp.logical_not(has_neighbour(side)))
            def _():
                taps[pl.ds(row * width, width), :] = jnp.zeros((width, 3 * mid), jnp.bfloat16)

        def edge_step(i, carry):
            return fold(carry, conv(i * (rows - 1), 1))

        carry = lax.fori_loop(0, 2, edge_step, carry)
        send_stats(first + 1, carry)

        scale, shift = affine(first + 1, gain_mid[layer, 1:2], shift_mid[layer, 1:2])

        def inner_step(i, _):
            at = pl.ds(i * width, width)
            inner[at, :] = jnp.maximum(red[at, :] * scale + shift, 0.0).astype(jnp.bfloat16)
            return 0

        lax.fori_loop(0, rows, inner_step, 0)

        weight_copy(2, layer).wait()
        for c in range(chunks):
            cols = slice(c * mid, (c + 1) * mid)

            def expand_step(i, carry):
                at = pl.ds(i * step * width, step * width)
                y = jnp.dot(
                    inner[at, :], we[layer, :, cols], preferred_element_type=jnp.float32
                )
                expanded[at, cols] = y
                return fold(carry, y)

            send_stats(first + 2 + c, lax.fori_loop(0, rows // step, expand_step, zeros()))

        for c in range(chunks):
            cols = slice(c * mid, (c + 1) * mid)
            scale, shift = affine(
                first + 2 + c,
                gain_out[pl.ds(layer, 1), cols],
                shift_out[pl.ds(layer, 1), cols],
            )

            def output_step(i, _):
                y = expanded[pl.ds(i * width, width), cols] * scale + shift
                y = y + x[i, :, cols].astype(jnp.float32)
                x[i, :, cols] = jnp.maximum(y, 0.0).astype(jnp.bfloat16)
                return 0

            lax.fori_loop(0, rows, output_step, 0)

            @pl.when(layer == layers - 1)
            def _():
                out_copy(c).start()

        return 0

    lax.fori_loop(0, layers, layer_step, 0)
    for c in range(chunks):
        out_copy(c).wait()


def solution(mesh):
    n = mesh.shape["slab"]

    def local(section_input, w_reduce, w_spatial, w_expand, gain_mid, shift_mid, gain_out, shift_out):
        rows, width, chans = section_input.shape
        layers, _, mid = w_reduce.shape
        chunks = chans // mid
        total = layers * (2 + chunks)
        bf16, f32 = jnp.bfloat16, jnp.float32
        hbm = pl.BlockSpec(memory_space=pl.ANY)
        vmem = pl.BlockSpec(memory_space=pltpu.VMEM)
        return pl.pallas_call(
            functools.partial(kernel, n),
            out_shape=jax.ShapeDtypeStruct(section_input.shape, bf16),
            in_specs=[hbm] * 4 + [vmem] * 4,
            out_specs=hbm,
            scratch_shapes=[
                pltpu.VMEM((rows, width, chans), bf16),
                pltpu.VMEM(w_reduce.shape, bf16),
                pltpu.VMEM(w_spatial.shape, bf16),
                pltpu.VMEM(w_expand.shape, bf16),
                pltpu.VMEM((rows * width, mid), f32),
                pltpu.VMEM(((rows + 2) * width, 3 * mid), bf16),
                pltpu.VMEM((rows * width, mid), bf16),
                pltpu.VMEM((rows * width, chans), f32),
                pltpu.VMEM((layers, 2, width, mid), bf16),
                pltpu.VMEM((layers, 2, width, mid), bf16),
                pltpu.VMEM((total, 2, mid), f32),
                pltpu.VMEM((total, n, 2, mid), f32),
                pltpu.SemaphoreType.DMA((rows,)),
                pltpu.SemaphoreType.DMA((3, layers)),
                pltpu.SemaphoreType.DMA((chunks,)),
                pltpu.SemaphoreType.DMA((layers, 2)),
                pltpu.SemaphoreType.DMA((layers, 2)),
                pltpu.SemaphoreType.DMA((total, n)),
                pltpu.SemaphoreType.DMA((total, n)),
            ],
            compiler_params=pltpu.CompilerParams(
                collective_id=0, has_side_effects=True, vmem_limit_bytes=56 * 1024 * 1024
            ),
            name="blocks",
        )(section_input, w_reduce, w_spatial, w_expand, gain_mid, shift_mid, gain_out, shift_out)

    placed = (P(("img", "slab"), None, None), P(), P(), P(), P(), P(), P(), P())
    return jax.shard_map(
        local, mesh=mesh, in_specs=placed, out_specs=P(("img", "slab"), None, None), check_vma=False
    )
```

```python
import functools

import jax
import jax.numpy as jnp
from jax import lax
from jax.experimental import pallas as pl
from jax.experimental.pallas import tpu as pltpu
from jax.sharding import PartitionSpec as P

MESH = pl.DeviceIdType.MESH
EPS = 1e-05
REDUCE_ROWS = 2
CONV_ROWS = 6
EXPAND_ROWS = 8
OUTPUT_ROWS = 4


def divisor(rows, most):
    return max(d for d in range(1, most + 1) if rows % d == 0)


def kernel(
    n, x_hbm, wr_hbm, ws_hbm, we_hbm, gain_mid, shift_mid, gain_out, shift_out, out_hbm,
    x, wr, ws, we, red, taps, inner, expanded, halo_out, halo_in, stat_out, stat, sums,
    x_sem, w_sem, out_sem, halo_send, halo_recv, stat_send, stat_recv,
):
    rows, width, chans = x.shape
    layers, _, mid = wr.shape
    chunks = chans // mid
    stages = 2 + chunks
    reduce_rows = divisor(rows, REDUCE_ROWS)
    conv_rows = divisor(rows - 2, CONV_ROWS)
    expand_rows = divisor(rows, EXPAND_ROWS)
    output_rows = divisor(rows, OUTPUT_ROWS)
    me = lax.axis_index("slab")
    inv_local = 1.0 / (rows * width)
    inv_count = 1.0 / (rows * width * n)

    def peer(k):
        return lax.rem(me + k, n)

    barrier = pltpu.get_barrier_semaphore()
    for k in range(1, n):
        pl.semaphore_signal(barrier, inc=1, device_id={"slab": peer(k)}, device_id_type=MESH)

    def weight_copy(kind, layer):
        source, target = ((wr_hbm, wr), (ws_hbm, ws), (we_hbm, we))[kind]
        return pltpu.make_async_copy(source.at[layer], target.at[layer], w_sem.at[kind, layer])

    def x_copy(row):
        return pltpu.make_async_copy(x_hbm.at[row], x.at[row], x_sem.at[row])

    def out_copy(chunk):
        cols = pl.ds(chunk * mid, mid)
        return pltpu.make_async_copy(x.at[:, :, cols], out_hbm.at[:, :, cols], out_sem.at[chunk])

    weight_copy(0, 0).start()
    for row in range(rows):
        x_copy(row).start()

    def stat_copy(stage, k):
        return pltpu.make_async_remote_copy(
            src_ref=stat_out.at[stage],
            dst_ref=stat.at[stage, me],
            send_sem=stat_send.at[stage, k],
            recv_sem=stat_recv.at[stage, me],
            device_id={"slab": peer(k)},
            device_id_type=MESH,
        )

    def stat_arrival(stage, k):
        source = peer(k)
        return pltpu.make_async_remote_copy(
            src_ref=stat_out.at[stage],
            dst_ref=stat.at[stage, source],
            send_sem=stat_send.at[stage, k],
            recv_sem=stat_recv.at[stage, source],
            device_id={"slab": source},
            device_id_type=MESH,
        )

    def fold(carry, y):
        total, squares = carry
        y = y.reshape(-1, 8, mid)
        return total + jnp.sum(y, axis=0), squares + jnp.sum(y * y, axis=0)

    def zeros():
        return jnp.zeros((8, mid), jnp.float32), jnp.zeros((8, mid), jnp.float32)

    def send_stats(stage, carry):
        total = jnp.sum(carry[0], axis=0, keepdims=True)
        squares = jnp.sum(carry[1], axis=0, keepdims=True)
        both = jnp.concatenate([total, squares], axis=0)
        stat_out[stage] = both
        stat[stage, me] = both
        for k in range(1, n):
            stat_copy(stage, k).start()
        return total

    def affine(stage, gain, shift):
        for k in range(1, n):
            stat_copy(stage, k).wait_send()
            stat_arrival(stage, k).wait_recv()
        both = jnp.sum(stat[stage], axis=0)
        mean = both[0:1] * inv_count
        var = jnp.maximum(both[1:2] * inv_count - mean * mean, 0.0)
        scale = lax.rsqrt(var + EPS) * gain
        return scale, shift - mean * scale

    def halo_copy(layer, side):
        return pltpu.make_async_remote_copy(
            src_ref=halo_out.at[layer, side],
            dst_ref=halo_in.at[layer, 1 - side],
            send_sem=halo_send.at[layer, side],
            recv_sem=halo_recv.at[layer, 1 - side],
            device_id={"slab": peer(n - 1 if side == 0 else 1)},
            device_id_type=MESH,
        )

    def halo_arrival(layer, side):
        return pltpu.make_async_remote_copy(
            src_ref=halo_out.at[layer, side],
            dst_ref=halo_in.at[layer, side],
            send_sem=halo_send.at[layer, side],
            recv_sem=halo_recv.at[layer, side],
            device_id={"slab": peer(n - 1 if side == 0 else 1)},
            device_id_type=MESH,
        )

    def has_neighbour(side):
        return me > 0 if side == 0 else me < n - 1

    column = lax.broadcasted_iota(jnp.int32, (width, mid), 0)

    def store_taps(row, h):
        at = pl.ds(row * width, width)
        before = jnp.where(column == 0, 0.0, pltpu.roll(h, 1, 0))
        after = jnp.where(column == width - 1, 0.0, pltpu.roll(h, width - 1, 0))
        taps[at, 0:mid] = before.astype(jnp.bfloat16)
        taps[at, mid : 2 * mid] = h.astype(jnp.bfloat16)
        taps[at, 2 * mid : 3 * mid] = after.astype(jnp.bfloat16)

    def keep_sums(carry):
        sums[0] = carry[0]
        sums[1] = carry[1]

    def reduce_step(i, carry):
        for r in range(reduce_rows):
            x_copy(i * reduce_rows + r).wait()
        y = jnp.dot(
            x[pl.ds(i * reduce_rows, reduce_rows)].reshape(reduce_rows * width, chans),
            wr[0],
            preferred_element_type=jnp.float32,
        )
        red[pl.ds(i * reduce_rows * width, reduce_rows * width), :] = y
        return fold(carry, y)

    weight_copy(0, 0).wait()
    keep_sums(lax.fori_loop(0, rows // reduce_rows, reduce_step, zeros()))
    pl.semaphore_wait(barrier, n - 1)

    def layer_step(layer, _):
        first = layer * stages

        carry = (sums[0], sums[1])
        local_mean = send_stats(first, carry) * inv_local
        for side in range(2):
            row = 0 if side == 0 else rows - 1
            halo_out[layer, side] = (red[row * width : (row + 1) * width, :] - local_mean).astype(
                jnp.bfloat16
            )

            @pl.when(has_neighbour(side))
            def _():
                halo_copy(layer, side).start()

        weight_copy(1, layer).start()
        weight_copy(2, layer).start()

        @pl.when(layer < layers - 1)
        def _():
            weight_copy(0, layer + 1).start()

        scale, shift = affine(first, gain_mid[layer, 0:1], shift_mid[layer, 0:1])

        def hidden_step(i, _):
            y = red[pl.ds(i * width, width), :]
            store_taps(i + 1, jnp.maximum(y * scale + shift, 0.0))
            return 0

        lax.fori_loop(0, rows, hidden_step, 0)

        weight_copy(1, layer).wait()

        def conv(row, count):
            total = None
            for down in range(3):
                part = jnp.dot(
                    taps[pl.ds((row + down) * width, count * width), :],
                    ws[layer, pl.ds(3 * down, 3)].reshape(3 * mid, mid),
                    preferred_element_type=jnp.float32,
                )
                total = part if total is None else total + part
            red[pl.ds(row * width, count * width), :] = total
            return total

        def inside_step(i, carry):
            return fold(carry, conv(1 + i * conv_rows, conv_rows))

        carry = lax.fori_loop(0, (rows - 2) // conv_rows, inside_step, zeros())

        for side in range(2):
            source = peer(n - 1 if side == 0 else 1)
            row = 0 if side == 0 else rows + 1

            @pl.when(has_neighbour(side))
            def _():
                halo_copy(layer, side).wait_send()
                halo_arrival(layer, side).wait_recv()
                theirs = stat[first, source][0:1] * inv_local
                y = halo_in[layer, side].astype(jnp.float32) + theirs
                store_taps(row, jnp.maximum(y * scale + shift, 0.0))

            @pl.when(jnp.logical_not(has_neighbour(side)))
            def _():
                taps[pl.ds(row * width, width), :] = jnp.zeros((width, 3 * mid), jnp.bfloat16)

        def edge_step(i, carry):
            return fold(carry, conv(i * (rows - 1), 1))

        carry = lax.fori_loop(0, 2, edge_step, carry)
        send_stats(first + 1, carry)

        scale, shift = affine(first + 1, gain_mid[layer, 1:2], shift_mid[layer, 1:2])

        weight_copy(2, layer).wait()
        for c in range(chunks):
            cols = slice(c * mid, (c + 1) * mid)

            def expand_step(i, carry):
                at = pl.ds(i * expand_rows * width, expand_rows * width)
                if c == 0:
                    block = jnp.maximum(red[at, :] * scale + shift, 0.0).astype(jnp.bfloat16)
                    inner[at, :] = block
                else:
                    block = inner[at, :]
                y = jnp.dot(block, we[layer, :, cols], preferred_element_type=jnp.float32)
                expanded[c, at, :] = y
                return fold(carry, y)

            send_stats(first + 2 + c, lax.fori_loop(0, rows // expand_rows, expand_step, zeros()))

        @pl.when(layer < layers - 1)
        def _():
            weight_copy(0, layer + 1).wait()

        for c in range(chunks):
            cols = slice(c * mid, (c + 1) * mid)
            scale, shift = affine(
                first + 2 + c,
                gain_out[pl.ds(layer, 1), cols],
                shift_out[pl.ds(layer, 1), cols],
            )

            def output(row, count):
                at = pl.ds(row * width, count * width)
                y = expanded[c, at, :] * scale + shift
                y = y + x[pl.ds(row, count), :, cols].reshape(count * width, mid).astype(jnp.float32)
                y = jnp.maximum(y, 0.0).astype(jnp.bfloat16)
                x[pl.ds(row, count), :, cols] = y.reshape(count, width, mid)
                return y

            @pl.when(layer < layers - 1)
            def _():
                def output_step(i, carry):
                    at = pl.ds(i * output_rows * width, output_rows * width)
                    y = jnp.dot(
                        output(i * output_rows, output_rows),
                        wr[layer + 1, cols, :],
                        preferred_element_type=jnp.float32,
                    )
                    if c > 0:
                        y = y + red[at, :]
                    red[at, :] = y
                    return fold(carry, y) if c == chunks - 1 else carry

                if c == chunks - 1:
                    keep_sums(lax.fori_loop(0, rows // output_rows, output_step, zeros()))
                else:
                    lax.fori_loop(0, rows // output_rows, output_step, 0)

            @pl.when(layer == layers - 1)
            def _():
                def output_step(i, _):
                    output(i, 1)
                    return 0

                lax.fori_loop(0, rows, output_step, 0)
                out_copy(c).start()

        return 0

    lax.fori_loop(0, layers, layer_step, 0)
    for c in range(chunks):
        out_copy(c).wait()


def solution(mesh):
    n = mesh.shape["slab"]

    def local(section_input, w_reduce, w_spatial, w_expand, gain_mid, shift_mid, gain_out, shift_out):
        rows, width, chans = section_input.shape
        layers, _, mid = w_reduce.shape
        chunks = chans // mid
        total = layers * (2 + chunks)
        bf16, f32 = jnp.bfloat16, jnp.float32
        hbm = pl.BlockSpec(memory_space=pl.ANY)
        vmem = pl.BlockSpec(memory_space=pltpu.VMEM)
        return pl.pallas_call(
            functools.partial(kernel, n),
            out_shape=jax.ShapeDtypeStruct(section_input.shape, bf16),
            in_specs=[hbm] * 4 + [vmem] * 4,
            out_specs=hbm,
            scratch_shapes=[
                pltpu.VMEM((rows, width, chans), bf16),
                pltpu.VMEM(w_reduce.shape, bf16),
                pltpu.VMEM(w_spatial.shape, bf16),
                pltpu.VMEM(w_expand.shape, bf16),
                pltpu.VMEM((rows * width, mid), f32),
                pltpu.VMEM(((rows + 2) * width, 3 * mid), bf16),
                pltpu.VMEM((rows * width, mid), bf16),
                pltpu.VMEM((chunks, rows * width, mid), f32),
                pltpu.VMEM((layers, 2, width, mid), bf16),
                pltpu.VMEM((layers, 2, width, mid), bf16),
                pltpu.VMEM((total, 2, mid), f32),
                pltpu.VMEM((total, n, 2, mid), f32),
                pltpu.VMEM((2, 8, mid), f32),
                pltpu.SemaphoreType.DMA((rows,)),
                pltpu.SemaphoreType.DMA((3, layers)),
                pltpu.SemaphoreType.DMA((chunks,)),
                pltpu.SemaphoreType.DMA((layers, 2)),
                pltpu.SemaphoreType.DMA((layers, 2)),
                pltpu.SemaphoreType.DMA((total, n)),
                pltpu.SemaphoreType.DMA((total, n)),
            ],
            compiler_params=pltpu.CompilerParams(
                collective_id=0, has_side_effects=True, vmem_limit_bytes=56 * 1024 * 1024
            ),
            name="blocks",
        )(section_input, w_reduce, w_spatial, w_expand, gain_mid, shift_mid, gain_out, shift_out)

    placed = (P(("img", "slab"), None, None), P(), P(), P(), P(), P(), P(), P())
    return jax.shard_map(
        local, mesh=mesh, in_specs=placed, out_specs=P(("img", "slab"), None, None), check_vma=False
    )
```
